16 devices in a mesh: fsdp: 16 (over z, y, x, core).
Axes of the slice: x: 2, y: 2, z: 2, core: 2. Of those that a mesh axis runs over, the one named last changes fastest.
Arguments:
- token_ids: int32 [64, 512], P('fsdp')
- grad_y: bfloat16 [64, 512, 896], P('fsdp')
- table: bfloat16 [151936, 896], P('fsdp')
- norm1_gain: bfloat16 [896], P('fsdp')
- norm2_gain: bfloat16 [896], P('fsdp')
- w_query: bfloat16 [896, 14, 64], P('fsdp')
- w_key: bfloat16 [896, 2, 64], P('fsdp')
- w_value: bfloat16 [896, 2, 64], P('fsdp')
- w_out: bfloat16 [896, 896], P('fsdp')
- w_gate: bfloat16 [896, 4864], P('fsdp')
- w_up: bfloat16 [896, 4864], P('fsdp')
- w_down: bfloat16 [4864, 896], P('fsdp')
Outputs:
- output 1: bfloat16 [64, 512, 896], P('fsdp')
- output 2: bfloat16 [151936, 896], P('fsdp')
- output 3: bfloat16 [896], P('fsdp')
- output 4: bfloat16 [896], P('fsdp')
- output 5: bfloat16 [896, 14, 64], P('fsdp')
- output 6: bfloat16 [896, 2, 64], P('fsdp')
- output 7: bfloat16 [896, 2, 64], P('fsdp')
- output 8: bfloat16 [896, 896], P('fsdp')
- output 9: bfloat16 [896, 4864], P('fsdp')
- output 10: bfloat16 [896, 4864], P('fsdp')
- output 11: bfloat16 [4864, 896], P('fsdp')
All inputs are finite; a program needn't handle non-finite values.
Results may differ from the reference program's by a relative error of at most 0.0156515.
Values are sent between devices in bfloat16 or wider.
A program may use at most 1 GiB of HBM per device.

```python
import jax
import jax.numpy as jnp
from jax import lax

VOCAB_SIZE = 151936
MODEL_DIM = 896
Q_HEADS = 14
KV_HEADS = 2
HEAD_DIM = 64
FFN_DIM = 4864
GLOBAL_BATCH = 64
SEQ_LEN = 512

NORM_EPS = 1e-5
ROPE_THETA = 500000.0
VOCAB_BITS = (VOCAB_SIZE - 1).bit_length()
TOKENS_ALL = GLOBAL_BATCH * SEQ_LEN


def draw_ids(rng_key):
    k_level, k_rank, k_flat, k_pick, k_perm = jax.random.split(rng_key, 5)
    id_shape = (GLOBAL_BATCH, SEQ_LEN)
    levels = jax.random.randint(k_level, id_shape, 0, VOCAB_BITS + 1)
    level_span = jnp.minimum(jnp.left_shift(jnp.ones(id_shape, jnp.int32), levels), VOCAB_SIZE)
    id_ranks = jax.random.randint(k_rank, id_shape, 0, level_span)
    flat_ids = jax.random.randint(k_flat, id_shape, 0, VOCAB_SIZE)
    use_flat = jax.random.randint(k_pick, id_shape, 0, 4) == 0
    id_ranks = jnp.where(use_flat, flat_ids, id_ranks)
    row_order = jax.random.permutation(k_perm, VOCAB_SIZE)
    return jnp.take(row_order, id_ranks).astype(jnp.int32)


def normal_weight(rng_key, w_shape, fan_in):
    return (jax.random.normal(rng_key, w_shape, jnp.float32) * fan_in ** -0.5).astype(jnp.bfloat16)


def setup_inputs(seed: int = 0) -> dict:
    keys = jax.random.split(jax.random.key(seed), 12)
    attn_width = Q_HEADS * HEAD_DIM
    return {
        "token_ids": draw_ids(keys[0]),
        "grad_y": (jax.random.normal(keys[1], (GLOBAL_BATCH, SEQ_LEN, MODEL_DIM), jnp.float32) * TOKENS_ALL ** -0.5).astype(jnp.bfloat16),
        "table": jax.random.normal(keys[2], (VOCAB_SIZE, MODEL_DIM), jnp.float32).astype(jnp.bfloat16),
        "norm1_gain": jax.random.uniform(keys[3], (MODEL_DIM,), jnp.float32, 0.5, 1.5).astype(jnp.bfloat16),
        "norm2_gain": jax.random.uniform(keys[4], (MODEL_DIM,), jnp.float32, 0.5, 1.5).astype(jnp.bfloat16),
        "w_query": normal_weight(keys[5], (MODEL_DIM, Q_HEADS, HEAD_DIM), MODEL_DIM),
        "w_key": normal_weight(keys[6], (MODEL_DIM, KV_HEADS, HEAD_DIM), MODEL_DIM),
        "w_value": normal_weight(keys[7], (MODEL_DIM, KV_HEADS, HEAD_DIM), MODEL_DIM),
        "w_out": normal_weight(keys[8], (attn_width, MODEL_DIM), attn_width),
        "w_gate": normal_weight(keys[9], (MODEL_DIM, FFN_DIM), MODEL_DIM),
        "w_up": normal_weight(keys[10], (MODEL_DIM, FFN_DIM), MODEL_DIM),
        "w_down": normal_weight(keys[11], (FFN_DIM, MODEL_DIM), FFN_DIM),
    }


def rms_norm(x_f32, gain_f32):
    inv_rms = lax.rsqrt(jnp.mean(x_f32 * x_f32, axis=-1, keepdims=True) + NORM_EPS)
    return (x_f32 * inv_rms * gain_f32).astype(jnp.bfloat16)


def rotary(x_f32):
    head_dim = x_f32.shape[-1]
    half_dim = head_dim // 2
    seq_len = x_f32.shape[-3]
    inv_freq = ROPE_THETA ** (-2.0 * jnp.arange(half_dim, dtype=jnp.float32) / head_dim)
    angles = jnp.arange(seq_len, dtype=jnp.float32)[:, None] * inv_freq[None, :]
    cos_tab = jnp.cos(angles)[:, None, :]
    sin_tab = jnp.sin(angles)[:, None, :]
    lo_half = x_f32[..., :half_dim]
    hi_half = x_f32[..., half_dim:]
    return jnp.concatenate([lo_half * cos_tab - hi_half * sin_tab, hi_half * cos_tab + lo_half * sin_tab], axis=-1)


def attend(q_f32, k_f32, v_bf16):
    q_rot = rotary(q_f32).astype(jnp.bfloat16).reshape(SEQ_LEN, KV_HEADS, Q_HEADS // KV_HEADS, HEAD_DIM)
    k_rot = rotary(k_f32).astype(jnp.bfloat16)
    scores = jnp.einsum("qkgd,skd->kgqs", q_rot.astype(jnp.float32), k_rot.astype(jnp.float32)) * HEAD_DIM ** -0.5
    positions = jnp.arange(SEQ_LEN)
    causal = positions[:, None] >= positions[None, :]
    scores = jnp.where(causal, scores, -1e30)
    prob_bf = jax.nn.softmax(scores, axis=-1).astype(jnp.bfloat16)
    attn_out = jnp.einsum("kgqs,skd->qkgd", prob_bf.astype(jnp.float32), v_bf16.astype(jnp.float32))
    return attn_out.astype(jnp.bfloat16).reshape(SEQ_LEN, Q_HEADS * HEAD_DIM)


def layer(emb_rows, gain_one, gain_two, w_query, w_key, w_value, w_out, w_gate, w_up, w_down):
    x_f32 = emb_rows.astype(jnp.float32)
    h_one = rms_norm(x_f32, gain_one).astype(jnp.float32)
    q_f32 = jnp.einsum("sd,dhe->she", h_one, w_query)
    k_f32 = jnp.einsum("sd,dhe->she", h_one, w_key)
    v_bf16 = jnp.einsum("sd,dhe->she", h_one, w_value).astype(jnp.bfloat16)
    attn_out = attend(q_f32, k_f32, v_bf16)
    resid_f32 = x_f32 + jnp.dot(attn_out.astype(jnp.float32), w_out, preferred_element_type=jnp.float32)
    resid_two = resid_f32.astype(jnp.bfloat16).astype(jnp.float32)
    h_two = rms_norm(resid_two, gain_two).astype(jnp.float32)
    gate_f32 = jnp.dot(h_two, w_gate, preferred_element_type=jnp.float32)
    up_f32 = jnp.dot(h_two, w_up, preferred_element_type=jnp.float32)
    act_f32 = (jax.nn.silu(gate_f32) * up_f32).astype(jnp.bfloat16).astype(jnp.float32)
    return (resid_two + jnp.dot(act_f32, w_down, preferred_element_type=jnp.float32)).astype(jnp.bfloat16)


def reference(token_ids, grad_y, table, norm1_gain, norm2_gain, w_query, w_key, w_value, w_out, w_gate, w_up, w_down):
    params = tuple(weight.astype(jnp.float32) for weight in (norm1_gain, norm2_gain, w_query, w_key, w_value, w_out, w_gate, w_up, w_down))

    def one_sequence(grad_acc, seq_in):
        seq_ids, seq_dy = seq_in
        emb_rows = jnp.take(table, seq_ids, axis=0)
        layer_out, pullback = jax.vjp(layer, emb_rows, *params)
        cotangents = pullback(seq_dy)
        new_acc = tuple(acc_old + cot_new for acc_old, cot_new in zip(grad_acc, cotangents[1:]))
        return new_acc, (layer_out, cotangents[0])

    zero_acc = tuple(jnp.zeros_like(weight) for weight in params)
    grad_acc, (y_out, d_emb) = lax.scan(one_sequence, zero_acc, (token_ids, grad_y))
    grad_table = jax.ops.segment_sum(d_emb.reshape(-1, MODEL_DIM).astype(jnp.float32), token_ids.reshape(-1), num_segments=VOCAB_SIZE).astype(jnp.bfloat16)
    grads = [acc_val.astype(jnp.bfloat16) for acc_val in grad_acc]
    return (y_out, grad_table, grads[0], grads[1], grads[2], grads[3], grads[4], grads[5], grads[6], grads[7], grads[8])
```

```python
import jax
import jax.numpy as jnp
from jax import lax
from jax.sharding import PartitionSpec as P

AXIS_NAME = "fsdp"
NORM_EPS = 1e-5
ROPE_THETA = 500000.0
N_DEV = 16
SLOTS = 128
RING = (0, 1, 2, 3, 6, 7, 4, 5, 12, 13, 14, 15, 10, 11, 8, 9)
F32 = jnp.float32
BF16 = jnp.bfloat16


def rms_norm(x_f32, gain_f32):
    inv_rms = lax.rsqrt(jnp.mean(x_f32 * x_f32, axis=-1, keepdims=True) + NORM_EPS)
    return (x_f32 * inv_rms * gain_f32).astype(BF16)


def rotary(x_f32):
    head_dim = x_f32.shape[-1]
    half_dim = head_dim // 2
    seq_len = x_f32.shape[-3]
    inv_freq = ROPE_THETA ** (-2.0 * jnp.arange(half_dim, dtype=F32) / head_dim)
    angles = jnp.arange(seq_len, dtype=F32)[:, None] * inv_freq[None, :]
    cos_tab = jnp.cos(angles)[:, None, :]
    sin_tab = jnp.sin(angles)[:, None, :]
    lo_half = x_f32[..., :half_dim]
    hi_half = x_f32[..., half_dim:]
    return jnp.concatenate([lo_half * cos_tab - hi_half * sin_tab, hi_half * cos_tab + lo_half * sin_tab], axis=-1)


def attend(q_f32, k_f32, v_bf16):
    batch_loc, seq_len, q_heads, head_dim = q_f32.shape
    kv_heads = k_f32.shape[2]
    q_rot = rotary(q_f32).astype(BF16).reshape(batch_loc, seq_len, kv_heads, q_heads // kv_heads, head_dim)
    k_rot = rotary(k_f32).astype(BF16)
    scores = jnp.einsum("bqkgd,bskd->bkgqs", q_rot, k_rot, preferred_element_type=F32) * head_dim ** -0.5
    positions = jnp.arange(seq_len)
    causal = positions[:, None] >= positions[None, :]
    scores = jnp.where(causal, scores, -1e30)
    prob_bf = jax.nn.softmax(scores, axis=-1).astype(BF16)
    attn_out = jnp.einsum("bkgqs,bskd->bqkgd", prob_bf, v_bf16, preferred_element_type=F32)
    return attn_out.astype(BF16).reshape(batch_loc, seq_len, q_heads * head_dim)


def gated(gate_f32, up_f32):
    return (jax.nn.silu(gate_f32) * up_f32).astype(BF16)


def mm(a, b):
    return jnp.dot(a, b, preferred_element_type=F32)


def mm_tn(a, b):
    return lax.dot_general(a, b, (((0,), (0,)), ((), ())), preferred_element_type=F32)


def mm_nt(a, b):
    return lax.dot_general(a, b, (((1,), (1,)), ((), ())), preferred_element_type=F32)


def ring_scatter(partial):
    return lax.psum_scatter(partial, AXIS_NAME, scatter_dimension=0, tiled=True, axis_index_groups=[list(RING)])


def to_owner(ring_block):
    return lax.ppermute(ring_block.astype(BF16), AXIS_NAME, [(RING[j], j) for j in range(N_DEV)])


def to_all(mine):
    copies = jnp.broadcast_to(mine[None], (N_DEV,) + mine.shape).reshape((-1,) + mine.shape[1:])
    return lax.all_to_all(copies, AXIS_NAME, 0, 0, tiled=True)


def plan_requests(ids, rows_dev):
    n_tok = ids.shape[0]
    owner = ids // rows_dev
    pos = jnp.arange(n_tok, dtype=jnp.int32)
    first = jnp.min(jnp.where(ids[:, None] == ids[None, :], pos[None, :], n_tok), axis=1)
    lead_owner = jnp.where(first == pos, owner, -1)
    rank = jnp.sum((lead_owner[None, :] == owner[:, None]) & (pos[None, :] < first[:, None]), axis=1, dtype=jnp.int32)
    slot = jnp.where(rank < SLOTS, owner * SLOTS + rank, N_DEV * SLOTS)
    lead_slot = jnp.where(first == pos, slot, N_DEV * SLOTS)
    local_row = ids - owner * rows_dev
    slots = jnp.arange(N_DEV * SLOTS, dtype=jnp.int32)
    asked = jnp.sum(jnp.where(lead_slot[None, :] == slots[:, None], local_row[None, :], 0), axis=1, dtype=jnp.int32)
    spill = jnp.any(rank >= SLOTS).astype(jnp.int32)
    return slot, asked, spill


def solution(mesh):
    spec_1d = P(AXIS_NAME)
    spec_2d = P(AXIS_NAME, None)
    spec_3d = P(AXIS_NAME, None, None)
    in_specs = (spec_2d, spec_3d, spec_2d, spec_1d, spec_1d, spec_3d, spec_3d, spec_3d, spec_2d, spec_2d, spec_2d, spec_2d)
    out_specs = (spec_3d, spec_2d, spec_1d, spec_1d, spec_3d, spec_3d, spec_3d, spec_2d, spec_2d, spec_2d, spec_2d)

    def device_step(token_ids, grad_y, table, norm1, norm2, w_query, w_key, w_value, w_out, w_gate, w_up, w_down):
        batch_loc, seq_len = token_ids.shape
        rows_dev, dim = table.shape
        n_tok = batch_loc * seq_len
        q_heads, head_dim = w_query.shape[1:]
        kv_heads = w_key.shape[1]
        ffn = w_gate.shape[1]
        shard = w_query.shape[0]
        q_w, kv_w = q_heads * head_dim, kv_heads * head_dim
        me = lax.axis_index(AXIS_NAME)

        ids = token_ids.reshape(n_tok)
        slot, asked, spill = plan_requests(ids, rows_dev)
        ask_row = jnp.concatenate([asked.reshape(N_DEV, SLOTS), jnp.full((1, SLOTS), spill, jnp.int32)], axis=0)
        ask_all = lax.all_gather(ask_row, AXIS_NAME, axis=0)
        asked_of_me = lax.dynamic_index_in_dim(ask_all, me, axis=1, keepdims=False).reshape(N_DEV * SLOTS)
        any_spill = jnp.max(ask_all[:, N_DEV, 0]) > 0

        gains_col = jnp.pad(jnp.stack([norm1, norm2], axis=1), ((0, 0), (0, 126)))
        pack_a = jnp.concatenate([w_query.reshape(shard, q_w), w_key.reshape(shard, kv_w), w_value.reshape(shard, kv_w), gains_col], axis=1)
        pack_b = jnp.concatenate([w_gate, w_up], axis=1)
        w_a = lax.all_gather(pack_a, AXIS_NAME, axis=0, tiled=True)
        w_o = lax.all_gather(w_out, AXIS_NAME, axis=0, tiled=True)
        w_d = lax.all_gather(w_down, AXIS_NAME, axis=0, tiled=True)
        w_gu = lax.all_gather(pack_b, AXIS_NAME, axis=0, tiled=True)
        w_qkv = w_a[:, : q_w + 2 * kv_w]
        gain_one = w_a[:, q_w + 2 * kv_w].astype(F32)
        gain_two = w_a[:, q_w + 2 * kv_w + 1].astype(F32)

        sent_rows = jnp.take(table, asked_of_me, axis=0)
        got_rows = lax.all_to_all(sent_rows, AXIS_NAME, 0, 0, tiled=True)

        def rows_short(args):
            return jnp.take(args[0], jnp.minimum(args[1], N_DEV * SLOTS - 1), axis=0)

        def rows_dense(args):
            ids_all = to_all(args[2])
            rel_ids = ids_all - me * rows_dev
            owned = (rel_ids >= 0) & (rel_ids < rows_dev)
            picked = jnp.take(args[3], jnp.where(owned, rel_ids, 0), axis=0)
            part = jnp.where(owned[:, None], picked, jnp.zeros((), BF16))
            parts = lax.all_to_all(part, AXIS_NAME, 0, 0, tiled=True).reshape(N_DEV, n_tok, dim)
            return jnp.sum(parts.astype(F32), axis=0).astype(BF16)

        x_bf = lax.cond(any_spill, rows_dense, rows_short, (got_rows, slot, ids, table))

        dy = grad_y.reshape(n_tok, dim)
        x_f32 = x_bf.astype(F32)
        h_one, norm1_pull = jax.vjp(rms_norm, x_f32, gain_one)
        qkv = mm(h_one, w_qkv)
        q_f32 = qkv[:, :q_w].reshape(batch_loc, seq_len, q_heads, head_dim)
        k_f32 = qkv[:, q_w : q_w + kv_w].reshape(batch_loc, seq_len, kv_heads, head_dim)
        v_bf16 = qkv[:, q_w + kv_w :].astype(BF16).reshape(batch_loc, seq_len, kv_heads, head_dim)
        attn_out, attn_pull = jax.vjp(attend, q_f32, k_f32, v_bf16)
        attn_flat = attn_out.reshape(n_tok, q_w)
        resid_two = (x_f32 + mm(attn_flat, w_o)).astype(BF16).astype(F32)
        h_two, norm2_pull = jax.vjp(rms_norm, resid_two, gain_two)
        gate_f32 = mm(h_two, w_gu[:, :ffn])
        up_f32 = mm(h_two, w_gu[:, ffn:])
        act_bf16, act_pull = jax.vjp(gated, gate_f32, up_f32)
        layer_out = (resid_two + mm(act_bf16, w_d)).astype(BF16)

        g_down = mm_tn(act_bf16, dy)
        d_act = mm_nt(dy, w_d).astype(BF16)
        d_gate, d_up = act_pull(d_act)
        d_gu = jnp.concatenate([d_gate.astype(BF16), d_up.astype(BF16)], axis=1)
        g_gu = mm_tn(h_two, d_gu)
        g_down, g_gu, d_gu = lax.optimization_barrier((g_down, g_gu, d_gu))
        sum_down = ring_scatter(g_down)
        sum_gu = ring_scatter(g_gu)
        d_h_two = mm_nt(d_gu, w_gu).astype(BF16)
        d_resid_two, g_norm2 = norm2_pull(d_h_two)
        d_resid = (dy.astype(F32) + d_resid_two).astype(BF16)
        g_out = mm_tn(attn_flat, d_resid)
        d_attn = mm_nt(d_resid, w_o).astype(BF16)
        d_query, d_key, d_value = attn_pull(d_attn.reshape(batch_loc, seq_len, q_w))
        d_qkv = jnp.concatenate([d_query.astype(BF16).reshape(n_tok, q_w), d_key.astype(BF16).reshape(n_tok, kv_w), d_value.reshape(n_tok, kv_w)], axis=1)
        g_qkv = mm_tn(h_one, d_qkv)
        d_h_one = mm_nt(d_qkv, w_qkv).astype(BF16)
        d_x, g_norm1 = norm1_pull(d_h_one)
        d_emb = (d_resid.astype(F32) + d_x).astype(BF16)
        g_norms = jnp.pad(jnp.stack([g_norm1, g_norm2], axis=1), ((0, 0), (0, 126)))

        chosen = (slot[:, None] == jnp.arange(N_DEV * SLOTS, dtype=jnp.int32)[None, :]).astype(BF16)
        slot_sums = mm_tn(chosen, d_emb)
        got_sums = lax.all_to_all(slot_sums, AXIS_NAME, 0, 0, tiled=True)
        g_rest = jnp.concatenate([g_qkv, g_norms, g_out], axis=1)
        g_rest, sum_down, sum_gu, got_sums = lax.optimization_barrier((g_rest, sum_down, sum_gu, got_sums))
        out_down, out_gu, out_rest = to_owner(sum_down), to_owner(sum_gu), to_owner(ring_scatter(g_rest))

        def table_short(args):
            acc = jnp.zeros((rows_dev, dim), F32).at[args[1]].add(args[0])
            return acc.astype(BF16)

        def table_dense(args):
            ids_all = to_all(args[2])
            rel_ids = ids_all - me * rows_dev
            owned = (rel_ids >= 0) & (rel_ids < rows_dev)
            d_all = to_all(args[3])
            seg_ids = jnp.where(owned, rel_ids, rows_dev)
            return jax.ops.segment_sum(d_all.astype(F32), seg_ids, num_segments=rows_dev).astype(BF16)

        d_table = lax.cond(any_spill, table_dense, table_short, (got_sums, asked_of_me, ids, d_emb))

        n_qkv = q_w + 2 * kv_w
        return (
            layer_out.reshape(batch_loc, seq_len, dim),
            d_table,
            out_rest[:, n_qkv],
            out_rest[:, n_qkv + 1],
            out_rest[:, :q_w].reshape(shard, q_heads, head_dim),
            out_rest[:, q_w : q_w + kv_w].reshape(shard, kv_heads, head_dim),
            out_rest[:, q_w + kv_w : n_qkv].reshape(shard, kv_heads, head_dim),
            out_rest[:, n_qkv + 128 :],
            out_gu[:, :ffn],
            out_gu[:, ffn:],
            out_down,
        )

    return jax.shard_map(device_step, mesh=mesh, in_specs=in_specs, out_specs=out_specs, check_vma=False)
```
